32 devices in a mesh: dp: 4 (over y, x), owner: 8 (over z, core).
Axes of the slice: x: 2, y: 2, z: 4, core: 2. Of those that a mesh axis runs over, the one named last changes fastest.
Arguments:
- partial_grads: bfloat16 [4, 48, 1024, 1024], P('dp', None, 'owner'), may hold values from -2.09375 to 2.09375
- owner_map: int32 [48], replicated, may hold values from 0 to 7, as said below
- left_stats: float32 [8, 12, 1024, 1024], P('owner', None, 'dp'), may hold values from -1.8 to 1.8
- right_stats: float32 [8, 12, 1024, 1024], P('owner', None, 'dp'), may hold values from -1.8 to 1.8
- left_roots: bfloat16 [8, 12, 1024, 1024], P('owner', None, 'dp'), as said below
- right_roots: bfloat16 [8, 12, 1024, 1024], P('owner', None, 'dp'), as said below
Outputs:
- direction: bfloat16 [48, 1024, 1024], P(None, ('dp', 'owner'))
- new_left_stats: float32 [8, 12, 1024, 1024], P('owner', None, 'dp')
- new_right_stats: float32 [8, 12, 1024, 1024], P('owner', None, 'dp')
The draws below stay inside these ranges and needn't reach their ends.
Inputs may be any that keep to these rules, and one draw needn't show every extreme that they name: `owner_map`: no owner index holds more than 12 blocks, and some owner holds exactly 12. `left_roots`: each block is dense and not symmetric; its diagonal entries are of order one and its off-diagonal entries are small. `right_roots`: each block is dense and not symmetric; its diagonal entries are of order one and its off-diagonal entries are small.
All inputs are finite; a program needn't handle non-finite values.
Results may differ from the reference program's by a relative error of at most 0.017.
Values may be sent and summed in bfloat16 or wider, within the bound.
A program may use at most 256 MiB of HBM per device.

```python
import jax
import jax.numpy as jnp
from jax import lax

D_MODEL = 2560
D_IN = 10576
D_INNER = 5120
TILE = 1024
TILES = 48
OWNERS = 8
SLOTS = 12
N_DP = 4


def draw_owner_map(key, part):
    first, second = jax.random.split(jax.random.fold_in(key, 7))
    total = OWNERS * SLOTS
    ranks = jax.random.permutation(first, total).astype(jnp.int32)
    chosen = jax.random.randint(second, (), 0, OWNERS, dtype=jnp.int32)
    ids = jnp.arange(total, dtype=jnp.int32)
    keyed = jnp.where(ids // SLOTS == chosen, -1 - ids % SLOTS, ranks)
    order = jnp.argsort(keyed, stable=True).astype(jnp.int32)
    return (order[:TILES] // SLOTS).astype(jnp.int32)


def draw_root(key):
    first, second = jax.random.split(key)
    shape = (OWNERS, SLOTS, TILE, TILE)
    diag = jax.random.uniform(first, (OWNERS, SLOTS, TILE), jnp.float32, 0.5, 1.5)
    off = jax.random.normal(second, shape, jnp.float32) * (0.4 / TILE ** 0.5)
    eye = jnp.eye(TILE, dtype=jnp.float32)
    return off + diag[..., None] * eye


def draw_left_roots(key, part):
    return draw_root(jax.random.fold_in(key, 11)).astype(jnp.bfloat16)


def draw_right_roots(key, part):
    return draw_root(jax.random.fold_in(key, 13)).astype(jnp.bfloat16)


def shard_levels(own_key, shape, shards, least, high):
    level = 1.0
    for position, shards_of in shards:
        draws = jax.random.uniform(jax.random.fold_in(jax.random.fold_in(own_key, 6), position), (shards_of,), jnp.float32, least / len(shards), high / len(shards))
        level = level * jnp.repeat(jnp.exp(draws), shape[position] // shards_of).reshape((-1,) + (1,) * (len(shape) - 1 - position))
    return level


def centred(key, shape, deviation, limit, shards=(), kind=jnp.bfloat16):
    values = deviation * jax.random.normal(key, shape, jnp.float32)
    if shards:
        values = values * shard_levels(key, shape, shards, -0.22, 0.18)
    return jnp.clip(values, -limit, limit).astype(kind)


def setup_inputs(seed: int = 0) -> dict:
    key_of = jax.random.split(jax.random.key(seed), 7)
    partial_grads = centred(key_of[0], (N_DP, TILES, TILE, TILE), 0.35, 2.09375, ((0, 4), (2, 8)))
    owner_map = draw_owner_map(jax.random.fold_in(key_of[6], 71), 0)
    left_stats = centred(key_of[2], (OWNERS, SLOTS, TILE, TILE), 0.3, 1.8, ((0, 8), (2, 4)), jnp.float32)
    right_stats = centred(key_of[3], (OWNERS, SLOTS, TILE, TILE), 0.3, 1.8, ((0, 8), (2, 4)), jnp.float32)
    left_roots = draw_left_roots(jax.random.fold_in(key_of[6], 71), 0)
    right_roots = draw_right_roots(jax.random.fold_in(key_of[6], 71), 0)
    return {"partial_grads": partial_grads, "owner_map": owner_map, "left_stats": left_stats, "right_stats": right_stats, "left_roots": left_roots, "right_roots": right_roots}


stat_decay = 0.999


def extents(count):
    index = jnp.arange(count, dtype=jnp.int32)
    in_cols = -(-D_IN // TILE)
    out_cols = -(-D_MODEL // TILE)
    in_count = (-(-D_MODEL // TILE)) * in_cols
    is_in = index < in_count
    other = jnp.maximum(index - in_count, 0)
    rows = jnp.where(is_in, jnp.minimum(TILE, D_MODEL - (index // in_cols) * TILE), jnp.minimum(TILE, D_INNER - (other // out_cols) * TILE))
    cols = jnp.where(is_in, jnp.minimum(TILE, D_IN - (index % in_cols) * TILE), jnp.minimum(TILE, D_MODEL - (other % out_cols) * TILE))
    return rows.astype(jnp.int32), cols.astype(jnp.int32)


def reference(partial_grads, owner_map, left_stats, right_stats, left_roots, right_roots):
    rows, cols = extents(TILES)
    line = jnp.arange(TILE, dtype=jnp.int32)
    mask = (line[None, :, None] < rows[:, None, None]) & (line[None, None, :] < cols[:, None, None])
    total = jnp.zeros(partial_grads.shape[1:], jnp.float32)
    for source in range(N_DP):
        total = total + partial_grads[source].astype(jnp.float32)
    grads = jnp.where(mask, total, jnp.float32(0.0)).astype(jnp.bfloat16)
    ids = jnp.arange(TILES, dtype=jnp.int32)
    same = (owner_map[:, None] == owner_map[None, :]) & (ids[None, :] < ids[:, None])
    slot = jnp.sum(same.astype(jnp.int32), axis=1).astype(jnp.int32)

    def per_tile(index):
        grad = grads[index]
        owner = owner_map[index]
        place = slot[index]
        left_new = stat_decay * left_stats[owner, place] + (1.0 - stat_decay) * jnp.dot(grad, grad.T, preferred_element_type=jnp.float32)
        right_new = stat_decay * right_stats[owner, place] + (1.0 - stat_decay) * jnp.dot(grad.T, grad, preferred_element_type=jnp.float32)
        left_part = jnp.dot(left_roots[owner, place], grad, preferred_element_type=jnp.float32).astype(jnp.bfloat16)
        result = jnp.dot(left_part, right_roots[owner, place], preferred_element_type=jnp.float32)
        result = jnp.where(mask[index], result, jnp.float32(0.0)).astype(jnp.bfloat16)
        return left_new, right_new, result

    left_all, right_all, direction = lax.map(per_tile, ids)
    new_left = (stat_decay * left_stats).at[owner_map, slot].set(left_all)
    new_right = (stat_decay * right_stats).at[owner_map, slot].set(right_all)
    return (direction, new_left, new_right)
```

```python
import functools

import jax
import jax.numpy as jnp
from jax import lax
from jax.experimental import pallas as pl
from jax.experimental.pallas import tpu as pltpu
from jax.sharding import PartitionSpec as P


D_MODEL = 2560
D_IN = 10576
D_INNER = 5120
TILE = 1024

CHUNK = 3

stat_decay = 0.999


def extents(count):
    index = jnp.arange(count, dtype=jnp.int32)
    in_cols = -(-D_IN // TILE)
    out_cols = -(-D_MODEL // TILE)
    in_count = -(-D_MODEL // TILE) * in_cols
    is_in = index < in_count
    other = jnp.maximum(index - in_count, 0)
    rows = jnp.where(
        is_in,
        jnp.minimum(TILE, D_MODEL - index // in_cols * TILE),
        jnp.minimum(TILE, D_INNER - other // out_cols * TILE),
    )
    cols = jnp.where(
        is_in,
        jnp.minimum(TILE, D_IN - index % in_cols * TILE),
        jnp.minimum(TILE, D_MODEL - other % out_cols * TILE),
    )
    return (rows, cols)


def dot(a, b, dims):
    return lax.dot_general(a, b, (dims, ((), ())), preferred_element_type=jnp.float32)


def step_kernel(base, info, grads, roots, left_roots, left_stats, right_stats, *rest):
    direction, new_left, new_right, left_part = rest[-4:]
    dp, _, _, piece, width = grads.shape
    lanes, tile = left_stats.shape[1:]
    here = info[0]
    pieces = lanes // piece
    full = [grads[d].reshape(tile, width) for d in range(dp)]
    mine = grads[here].reshape(tile, width).T
    gram = None
    for d in range(dp):
        right = dot(mine, full[d], ((1,), (0,)))
        cut = (0, slice(None), slice(d * width, (d + 1) * width))
        new_right[cut] = stat_decay * right_stats[cut] + (1.0 - stat_decay) * right
        part = dot(left_roots[0], full[d], ((1,), (0,)))
        left_part[:, d * width : (d + 1) * width] = part.astype(jnp.bfloat16)
        rows = grads[d, pl.ds(here * pieces, pieces)].reshape(lanes, width)
        term = dot(rows, full[d], ((1,), (1,)))
        gram = term if gram is None else gram + term
    new_left[0] = stat_decay * left_stats[0] + (1.0 - stat_decay) * gram
    product = dot(left_part[...], roots[...].reshape(tile, tile), ((1,), (0,)))
    slot = base + pl.program_id(0)
    row = lax.broadcasted_iota(jnp.int32, product.shape, 0)
    col = lax.broadcasted_iota(jnp.int32, product.shape, 1)
    keep = (row < info[1 + 2 * slot]) & (col < info[2 + 2 * slot])
    result = jnp.where(keep, product, 0.0).astype(jnp.bfloat16)
    direction[...] = result.reshape(direction.shape)


def step(base, chunk, info, grads, roots, left_roots, left_stats, right_stats, carried):
    dp, owners, _, piece, width = grads.shape
    _, lanes, tile = left_stats.shape
    at = lambda s, info: (base + s, 0, 0)
    stats = pl.BlockSpec((1, lanes, tile), at)
    in_specs = [
        pl.BlockSpec((dp, owners, 1, piece, width), lambda s, info: (0, 0, s, 0, 0)),
        pl.BlockSpec((dp, 1, lanes, tile), lambda s, info: (0, base + s, 0, 0)),
        stats,
        stats,
        stats,
    ] + [pl.BlockSpec(memory_space=pl.ANY)] * len(carried)
    sub = lanes // owners
    return pl.pallas_call(
        functools.partial(step_kernel, base),
        grid_spec=pltpu.PrefetchScalarGridSpec(
            num_scalar_prefetch=1,
            grid=(chunk,),
            in_specs=in_specs,
            out_specs=[
                pl.BlockSpec((owners, 1, sub, tile), lambda s, info: (0, s, 0, 0)),
                stats,
                stats,
            ],
            scratch_shapes=[pltpu.VMEM((lanes, tile), jnp.bfloat16)],
        ),
        out_shape=[
            jax.ShapeDtypeStruct((owners, chunk, sub, tile), jnp.bfloat16),
            jax.ShapeDtypeStruct(left_stats.shape, jnp.float32),
            jax.ShapeDtypeStruct(right_stats.shape, jnp.float32),
        ],
        input_output_aliases={6: 1, 7: 2} if carried else {},
        compiler_params=pltpu.CompilerParams(vmem_limit_bytes=48 * 1024 * 1024),
        cost_estimate=pl.CostEstimate(
            flops=8 * chunk * lanes * tile * tile,
            bytes_accessed=chunk * (4 * tile * tile + 20 * lanes * tile),
            transcendentals=0,
        ),
    )(info, grads, roots, left_roots, left_stats, right_stats, *carried)


def inner(partial_grads, owner_map, left_stats, right_stats, left_roots, right_roots):
    dp = lax.axis_size("dp")
    owners = lax.axis_size("owner")
    owner_here = lax.axis_index("owner")
    dp_here = lax.axis_index("dp")
    tiles = owner_map.shape[0]
    slots = left_stats.shape[1]
    lanes = left_stats.shape[2]
    tile = left_stats.shape[3]
    piece = partial_grads.shape[2]
    width = tile // dp
    rows, cols = extents(tiles)
    ids = jnp.arange(tiles, dtype=jnp.int32)
    same = (owner_map[:, None] == owner_map[None, :]) & (ids[None, :] < ids[:, None])
    slot = jnp.sum(same.astype(jnp.int32), axis=1)
    picks = (slot[None, None, :] == jnp.arange(slots, dtype=jnp.int32)[None, :, None]) & (
        owner_map[None, None, :] == jnp.arange(owners, dtype=jnp.int32)[:, None, None]
    )
    tile_of = jnp.sum(jnp.where(picks, ids[None, None, :], 0), axis=2)
    filled = jnp.any(picks, axis=2)

    shares = lax.psum_scatter(partial_grads[0], "dp", scatter_dimension=2, tiled=True)
    roots = lax.all_gather(right_roots[0], "dp", axis=0)

    piece_rows = owner_here * piece + jnp.arange(piece, dtype=jnp.int32)
    piece_cols = dp_here * width + jnp.arange(width, dtype=jnp.int32)
    tile_here = lax.dynamic_index_in_dim(tile_of, owner_here, 0, keepdims=False)
    info = jnp.stack([jnp.take(rows, tile_here) - dp_here * lanes, jnp.take(cols, tile_here)], 1)
    info = jnp.concatenate([dp_here[None], info.reshape(-1)]).astype(jnp.int32)

    chunk = CHUNK if slots % CHUNK == 0 else 1
    arrived = []
    for base in range(0, slots, chunk):
        which = tile_of[:, base : base + chunk]
        rows_of = jnp.where(filled[:, base : base + chunk], jnp.take(rows, which), 0)
        mask = (piece_rows[:, None] < rows_of[:, :, None, None]) & (
            piece_cols[None, :] < jnp.take(cols, which)[:, :, None, None]
        )
        taken = jnp.take(shares, which.reshape(-1), axis=0).reshape(owners, chunk, piece, width)
        sent = lax.all_to_all(
            jnp.where(mask, taken, jnp.zeros((), shares.dtype)),
            "owner",
            split_axis=0,
            concat_axis=0,
            tiled=True,
        )
        arrived.append(sent)

    def place(index, returned, direction):
        flat = returned.reshape(owners * chunk, lanes // owners, tile)
        inside = slot // chunk == index
        at = jnp.where(inside, owner_map * chunk + slot - index * chunk, 0)
        return jnp.where(inside[:, None, None], jnp.take(flat, at, axis=0), direction)

    direction = jnp.zeros((tiles, lanes // owners, tile), jnp.bfloat16)
    carried = ()
    for index, base in enumerate(range(0, slots, chunk)):
        grads = lax.all_gather(arrived[index], "dp", axis=0)
        if index:
            grads, returned = lax.optimization_barrier((grads, returned))
            direction = place(index - 1, returned, direction)
        result, *carried = step(
            base, chunk, info, grads, roots, left_roots[0], left_stats[0], right_stats[0], carried
        )
        returned = lax.all_to_all(result, "owner", split_axis=0, concat_axis=0, tiled=True)
    direction = place(slots // chunk - 1, returned, direction)
    new_left, new_right = carried
    return (direction, new_left[None], new_right[None])


def solution(mesh):
    placed = (
        P("dp", None, "owner", None),
        P(),
        P("owner", None, "dp", None),
        P("owner", None, "dp", None),
        P("owner", None, "dp", None),
        P("owner", None, "dp", None),
    )
    return jax.shard_map(
        inner,
        mesh=mesh,
        in_specs=placed,
        out_specs=(
            P(None, ("dp", "owner"), None),
            P("owner", None, "dp", None),
            P("owner", None, "dp", None),
        ),
        check_vma=False,
    )
```

```python
import functools

import jax
import jax.numpy as jnp
from jax import lax
from jax.experimental import pallas as pl
from jax.experimental.pallas import tpu as pltpu
from jax.sharding import PartitionSpec as P


D_MODEL = 2560
D_IN = 10576
D_INNER = 5120
TILE = 1024

stat_decay = 0.999


def extents(count):
    index = jnp.arange(count, dtype=jnp.int32)
    in_cols = -(-D_IN // TILE)
    out_cols = -(-D_MODEL // TILE)
    in_count = -(-D_MODEL // TILE) * in_cols
    is_in = index < in_count
    other = jnp.maximum(index - in_count, 0)
    rows = jnp.where(
        is_in,
        jnp.minimum(TILE, D_MODEL - index // in_cols * TILE),
        jnp.minimum(TILE, D_INNER - other // out_cols * TILE),
    )
    cols = jnp.where(
        is_in,
        jnp.minimum(TILE, D_IN - index % in_cols * TILE),
        jnp.minimum(TILE, D_MODEL - other % out_cols * TILE),
    )
    return (rows, cols)


def dot(a, b, dims):
    return lax.dot_general(a, b, (dims, ((), ())), preferred_element_type=jnp.float32)


def step_kernel(base, info, grads, roots, left_roots, left_stats, right_stats, *rest):
    direction, new_left, new_right, left_part = rest[-4:]
    dp, _, _, piece, width = grads.shape
    lanes, tile = left_stats.shape[1:]
    here = info[0]
    pieces = lanes // piece
    full = [grads[d].reshape(tile, width) for d in range(dp)]
    mine = grads[here].reshape(tile, width).T
    gram = None
    for d in range(dp):
        right = dot(mine, full[d], ((1,), (0,)))
        cut = (0, slice(None), slice(d * width, (d + 1) * width))
        new_right[cut] = stat_decay * right_stats[cut] + (1.0 - stat_decay) * right
        part = dot(left_roots[0], full[d], ((1,), (0,)))
        left_part[:, d * width : (d + 1) * width] = part.astype(jnp.bfloat16)
        rows = grads[d, pl.ds(here * pieces, pieces)].reshape(lanes, width)
        term = dot(rows, full[d], ((1,), (1,)))
        gram = term if gram is None else gram + term
    new_left[0] = stat_decay * left_stats[0] + (1.0 - stat_decay) * gram
    product = dot(left_part[...], roots[...].reshape(tile, tile), ((1,), (0,)))
    slot = base + pl.program_id(0)
    row = lax.broadcasted_iota(jnp.int32, product.shape, 0)
    col = lax.broadcasted_iota(jnp.int32, product.shape, 1)
    keep = (row < info[1 + 2 * slot]) & (col < info[2 + 2 * slot])
    result = jnp.where(keep, product, 0.0).astype(jnp.bfloat16)
    direction[...] = result.reshape(direction.shape)


def step(base, chunk, info, grads, roots, left_roots, left_stats, right_stats, carried):
    dp, owners, _, piece, width = grads.shape
    _, lanes, tile = left_stats.shape
    at = lambda s, info: (base + s, 0, 0)
    stats = pl.BlockSpec((1, lanes, tile), at)
    in_specs = [
        pl.BlockSpec((dp, owners, 1, piece, width), lambda s, info: (0, 0, s, 0, 0)),
        pl.BlockSpec((dp, 1, lanes, tile), lambda s, info: (0, base + s, 0, 0)),
        stats,
        stats,
        stats,
    ] + [pl.BlockSpec(memory_space=pl.ANY)] * len(carried)
    sub = lanes // owners
    return pl.pallas_call(
        functools.partial(step_kernel, base),
        grid_spec=pltpu.PrefetchScalarGridSpec(
            num_scalar_prefetch=1,
            grid=(chunk,),
            in_specs=in_specs,
            out_specs=[
                pl.BlockSpec((owners, 1, sub, tile), lambda s, info: (0, s, 0, 0)),
                stats,
                stats,
            ],
            scratch_shapes=[pltpu.VMEM((lanes, tile), jnp.bfloat16)],
        ),
        out_shape=[
            jax.ShapeDtypeStruct((owners, chunk, sub, tile), jnp.bfloat16),
            jax.ShapeDtypeStruct(left_stats.shape, jnp.float32),
            jax.ShapeDtypeStruct(right_stats.shape, jnp.float32),
        ],
        input_output_aliases={6: 1, 7: 2} if carried else {},
        compiler_params=pltpu.CompilerParams(vmem_limit_bytes=48 * 1024 * 1024),
        cost_estimate=pl.CostEstimate(
            flops=8 * chunk * lanes * tile * tile,
            bytes_accessed=chunk * (4 * tile * tile + 20 * lanes * tile),
            transcendentals=0,
        ),
    )(info, grads, roots, left_roots, left_stats, right_stats, *carried)


def chunks_of(slots):
    if slots < 6:
        sizes = (slots,)
    else:
        last, middle = slots // 4, slots // 3
        sizes = (slots - middle - last, middle, last)
    return [(sum(sizes[:index]), size) for index, size in enumerate(sizes)]


def inner(partial_grads, owner_map, left_stats, right_stats, left_roots, right_roots):
    dp = lax.axis_size("dp")
    owners = lax.axis_size("owner")
    owner_here = lax.axis_index("owner")
    dp_here = lax.axis_index("dp")
    tiles = owner_map.shape[0]
    slots = left_stats.shape[1]
    lanes = left_stats.shape[2]
    tile = left_stats.shape[3]
    piece = partial_grads.shape[2]
    width = tile // dp
    rows, cols = extents(tiles)
    ids = jnp.arange(tiles, dtype=jnp.int32)
    same = (owner_map[:, None] == owner_map[None, :]) & (ids[None, :] < ids[:, None])
    slot = jnp.sum(same.astype(jnp.int32), axis=1)
    picks = (slot[None, None, :] == jnp.arange(slots, dtype=jnp.int32)[None, :, None]) & (
        owner_map[None, None, :] == jnp.arange(owners, dtype=jnp.int32)[:, None, None]
    )
    tile_of = jnp.sum(jnp.where(picks, ids[None, None, :], 0), axis=2)
    filled = jnp.any(picks, axis=2)

    shares = lax.psum_scatter(partial_grads[0], "dp", scatter_dimension=2, tiled=True)
    roots = lax.all_gather(right_roots[0], "dp", axis=0)

    piece_rows = owner_here * piece + jnp.arange(piece, dtype=jnp.int32)
    piece_cols = dp_here * width + jnp.arange(width, dtype=jnp.int32)
    tile_here = lax.dynamic_index_in_dim(tile_of, owner_here, 0, keepdims=False)
    info = jnp.stack([jnp.take(rows, tile_here) - dp_here * lanes, jnp.take(cols, tile_here)], 1)
    info = jnp.concatenate([dp_here[None], info.reshape(-1)]).astype(jnp.int32)

    spans = chunks_of(slots)
    arrived = []
    for base, chunk in spans:
        which = tile_of[:, base : base + chunk]
        rows_of = jnp.where(filled[:, base : base + chunk], jnp.take(rows, which), 0)
        mask = (piece_rows[:, None] < rows_of[:, :, None, None]) & (
            piece_cols[None, :] < jnp.take(cols, which)[:, :, None, None]
        )
        taken = jnp.take(shares, which.reshape(-1), axis=0).reshape(owners, chunk, piece, width)
        sent = lax.all_to_all(
            jnp.where(mask, taken, jnp.zeros((), shares.dtype)),
            "owner",
            split_axis=0,
            concat_axis=0,
            tiled=True,
        )
        arrived.append(sent)

    def place(index, returned, direction):
        base, chunk = spans[index]
        flat = returned.reshape(owners * chunk, lanes // owners, tile)
        inside = (slot >= base) & (slot < base + chunk)
        at = jnp.where(inside, owner_map * chunk + slot - base, 0)
        return jnp.where(inside[:, None, None], jnp.take(flat, at, axis=0), direction)

    direction = jnp.zeros((tiles, lanes // owners, tile), jnp.bfloat16)
    carried = ()
    for index, (base, chunk) in enumerate(spans):
        grads = lax.all_gather(arrived[index], "dp", axis=0)
        if index:
            direction = place(index - 1, returned, direction)
            grads, direction = lax.optimization_barrier((grads, direction))
        result, *carried = step(
            base, chunk, info, grads, roots, left_roots[0], left_stats[0], right_stats[0], carried
        )
        returned = lax.all_to_all(result, "owner", split_axis=0, concat_axis=0, tiled=True)
    direction = place(len(spans) - 1, returned, direction)
    new_left, new_right = carried
    return (direction, new_left[None], new_right[None])


def solution(mesh):
    placed = (
        P("dp", None, "owner", None),
        P(),
        P("owner", None, "dp", None),
        P("owner", None, "dp", None),
        P("owner", None, "dp", None),
        P("owner", None, "dp", None),
    )
    return jax.shard_map(
        inner,
        mesh=mesh,
        in_specs=placed,
        out_specs=(
            P(None, ("dp", "owner"), None),
            P("owner", None, "dp", None),
            P("owner", None, "dp", None),
        ),
        check_vma=False,
    )
```

```python
import functools

import jax
import jax.numpy as jnp
from jax import lax
from jax.experimental import pallas as pl
from jax.experimental.pallas import tpu as pltpu
from jax.sharding import PartitionSpec as P


D_MODEL = 2560
D_IN = 10576
D_INNER = 5120
TILE = 1024

stat_decay = 0.999


def extents(count):
    index = jnp.arange(count, dtype=jnp.int32)
    in_cols = -(-D_IN // TILE)
    out_cols = -(-D_MODEL // TILE)
    in_count = -(-D_MODEL // TILE) * in_cols
    is_in = index < in_count
    other = jnp.maximum(index - in_count, 0)
    rows = jnp.where(
        is_in,
        jnp.minimum(TILE, D_MODEL - index // in_cols * TILE),
        jnp.minimum(TILE, D_INNER - other // out_cols * TILE),
    )
    cols = jnp.where(
        is_in,
        jnp.minimum(TILE, D_IN - index % in_cols * TILE),
        jnp.minimum(TILE, D_MODEL - other % out_cols * TILE),
    )
    return (rows, cols)


def dot(a, b, dims):
    return lax.dot_general(a, b, (dims, ((), ())), preferred_element_type=jnp.float32)


def product_kernel(base, info, grads, roots, left_roots, direction, left_part):
    dp, _, _, _, width = grads.shape
    tile = roots.shape[-1]
    for d in range(dp):
        part = dot(left_roots[0], grads[d].reshape(tile, width), ((1,), (0,)))
        left_part[:, d * width : (d + 1) * width] = part.astype(jnp.bfloat16)
    product = dot(left_part[...], roots[...].reshape(tile, tile), ((1,), (0,)))
    slot = base + pl.program_id(0)
    row = lax.broadcasted_iota(jnp.int32, product.shape, 0)
    col = lax.broadcasted_iota(jnp.int32, product.shape, 1)
    keep = (row < info[1 + 2 * slot]) & (col < info[2 + 2 * slot])
    result = jnp.where(keep, product, 0.0).astype(jnp.bfloat16)
    direction[...] = result.reshape(direction.shape)


def stats_kernel(info, grads, left_stats, right_stats, *rest):
    new_left, new_right = rest[-2:]
    dp, _, _, piece, width = grads.shape
    lanes, tile = left_stats.shape[1:]
    here = info[0]
    pieces = lanes // piece
    full = [grads[d].reshape(tile, width) for d in range(dp)]
    mine = grads[here].reshape(tile, width).T
    gram = None
    for d in range(dp):
        right = dot(mine, full[d], ((1,), (0,)))
        cut = (0, slice(None), slice(d * width, (d + 1) * width))
        new_right[cut] = stat_decay * right_stats[cut] + (1.0 - stat_decay) * right
        rows = grads[d, pl.ds(here * pieces, pieces)].reshape(lanes, width)
        term = dot(rows, full[d], ((1,), (1,)))
        gram = term if gram is None else gram + term
    new_left[0] = stat_decay * left_stats[0] + (1.0 - stat_decay) * gram


def params():
    return pltpu.CompilerParams(vmem_limit_bytes=48 * 1024 * 1024)


def product_step(base, chunk, info, grads, roots, left_roots):
    dp, owners, _, piece, width = grads.shape
    _, lanes, tile = left_roots.shape
    sub = lanes // owners
    return pl.pallas_call(
        functools.partial(product_kernel, base),
        grid_spec=pltpu.PrefetchScalarGridSpec(
            num_scalar_prefetch=1,
            grid=(chunk,),
            in_specs=[
                pl.BlockSpec((dp, owners, 1, piece, width), lambda s, info: (0, 0, s, 0, 0)),
                pl.BlockSpec((dp, 1, lanes, tile), lambda s, info: (0, base + s, 0, 0)),
                pl.BlockSpec((1, lanes, tile), lambda s, info: (base + s, 0, 0)),
            ],
            out_specs=pl.BlockSpec((owners, 1, sub, tile), lambda s, info: (0, s, 0, 0)),
            scratch_shapes=[pltpu.VMEM((lanes, tile), jnp.bfloat16)],
        ),
        out_shape=jax.ShapeDtypeStruct((owners, chunk, sub, tile), jnp.bfloat16),
        compiler_params=params(),
        cost_estimate=pl.CostEstimate(
            flops=4 * chunk * lanes * tile * tile,
            bytes_accessed=chunk * (4 * tile * tile + 4 * lanes * tile),
            transcendentals=0,
        ),
    )(info, grads, roots, left_roots)


def stats_step(base, chunk, info, grads, left_stats, right_stats, carried):
    dp, owners, _, piece, width = grads.shape
    _, lanes, tile = left_stats.shape
    stats = pl.BlockSpec((1, lanes, tile), lambda s, info: (base + s, 0, 0))
    return pl.pallas_call(
        stats_kernel,
        grid_spec=pltpu.PrefetchScalarGridSpec(
            num_scalar_prefetch=1,
            grid=(chunk,),
            in_specs=[
                pl.BlockSpec((dp, owners, 1, piece, width), lambda s, info: (0, 0, s, 0, 0)),
                stats,
                stats,
            ]
            + [pl.BlockSpec(memory_space=pl.ANY)] * len(carried),
            out_specs=[stats, stats],
        ),
        out_shape=[
            jax.ShapeDtypeStruct(left_stats.shape, jnp.float32),
            jax.ShapeDtypeStruct(right_stats.shape, jnp.float32),
        ],
        input_output_aliases={4: 0, 5: 1} if carried else {},
        compiler_params=params(),
        cost_estimate=pl.CostEstimate(
            flops=4 * chunk * lanes * tile * tile,
            bytes_accessed=chunk * (2 * tile * tile + 16 * lanes * tile),
            transcendentals=0,
        ),
    )(info, grads, left_stats, right_stats, *carried)


def chunks_of(slots):
    if slots < 6:
        sizes = (slots,)
    else:
        last, middle = slots // 4, slots // 3
        sizes = (slots - middle - last, middle, last)
    return [(sum(sizes[:index]), size) for index, size in enumerate(sizes)]


def inner(partial_grads, owner_map, left_stats, right_stats, left_roots, right_roots):
    dp = lax.axis_size("dp")
    owners = lax.axis_size("owner")
    owner_here = lax.axis_index("owner")
    dp_here = lax.axis_index("dp")
    tiles = owner_map.shape[0]
    slots = left_stats.shape[1]
    lanes = left_stats.shape[2]
    tile = left_stats.shape[3]
    piece = partial_grads.shape[2]
    width = tile // dp
    rows, cols = extents(tiles)
    ids = jnp.arange(tiles, dtype=jnp.int32)
    same = (owner_map[:, None] == owner_map[None, :]) & (ids[None, :] < ids[:, None])
    slot = jnp.sum(same.astype(jnp.int32), axis=1)
    picks = (slot[None, None, :] == jnp.arange(slots, dtype=jnp.int32)[None, :, None]) & (
        owner_map[None, None, :] == jnp.arange(owners, dtype=jnp.int32)[:, None, None]
    )
    tile_of = jnp.sum(jnp.where(picks, ids[None, None, :], 0), axis=2)
    filled = jnp.any(picks, axis=2)

    shares = lax.psum_scatter(partial_grads[0], "dp", scatter_dimension=2, tiled=True)
    roots = lax.all_gather(right_roots[0], "dp", axis=0)

    piece_rows = owner_here * piece + jnp.arange(piece, dtype=jnp.int32)
    piece_cols = dp_here * width + jnp.arange(width, dtype=jnp.int32)
    tile_here = lax.dynamic_index_in_dim(tile_of, owner_here, 0, keepdims=False)
    info = jnp.stack([jnp.take(rows, tile_here) - dp_here * lanes, jnp.take(cols, tile_here)], 1)
    info = jnp.concatenate([dp_here[None], info.reshape(-1)]).astype(jnp.int32)

    spans = chunks_of(slots)
    arrived = []
    for base, chunk in spans:
        which = tile_of[:, base : base + chunk]
        rows_of = jnp.where(filled[:, base : base + chunk], jnp.take(rows, which), 0)
        mask = (piece_rows[:, None] < rows_of[:, :, None, None]) & (
            piece_cols[None, :] < jnp.take(cols, which)[:, :, None, None]
        )
        taken = jnp.take(shares, which.reshape(-1), axis=0).reshape(owners, chunk, piece, width)
        sent = lax.all_to_all(
            jnp.where(mask, taken, jnp.zeros((), shares.dtype)),
            "owner",
            split_axis=0,
            concat_axis=0,
            tiled=True,
        )
        arrived.append(sent)

    def place(index, returned, direction):
        base, chunk = spans[index]
        flat = returned.reshape(owners * chunk, lanes // owners, tile)
        inside = (slot >= base) & (slot < base + chunk)
        at = jnp.where(inside, owner_map * chunk + slot - base, 0)
        return jnp.where(inside[:, None, None], jnp.take(flat, at, axis=0), direction)

    direction = jnp.zeros((tiles, lanes // owners, tile), jnp.bfloat16)
    carried = ()
    for index, (base, chunk) in enumerate(spans):
        grads = lax.all_gather(arrived[index], "dp", axis=0)
        if index:
            grads, returned = lax.optimization_barrier((grads, returned))
        result = product_step(base, chunk, info, grads, roots, left_roots[0])
        if index:
            direction = place(index - 1, returned, direction)
        returned = lax.all_to_all(result, "owner", split_axis=0, concat_axis=0, tiled=True)
        grads, direction, result = lax.optimization_barrier((grads, direction, result))
        carried = stats_step(base, chunk, info, grads, left_stats[0], right_stats[0], carried)
    direction = place(len(spans) - 1, returned, direction)
    new_left, new_right = carried
    return (direction, new_left[None], new_right[None])


def solution(mesh):
    placed = (
        P("dp", None, "owner", None),
        P(),
        P("owner", None, "dp", None),
        P("owner", None, "dp", None),
        P("owner", None, "dp", None),
        P("owner", None, "dp", None),
    )
    return jax.shard_map(
        inner,
        mesh=mesh,
        in_specs=placed,
        out_specs=(
            P(None, ("dp", "owner"), None),
            P("owner", None, "dp", None),
            P("owner", None, "dp", None),
        ),
        check_vma=False,
    )
```
